256 devices in a mesh: merge: 4 (over y), row: 4 (over x_hi, core), col: 16 (over x_lo, z).
Axes of the slice: x: 4 (x_hi: 2, x_lo: 2; x = x_hi * 2 + x_lo), y: 4, z: 8, core: 2. Of those that a mesh axis runs over, the one named last changes fastest.
Arguments:
- eigen_rows: bfloat16 [4, 128, 16384], P('merge', 'row', 'col'), may hold values from -6 to 6
- live_one: int32 [4], replicated, may hold values from 2048 to 6144, as said below
- order_one: int32 [4, 16384], P('merge'), may hold values from 0 to 16383, each once within a row
- poles_one: float32 [4, 16384], P('merge'), may hold values from -2048 to 2048.3, as said below
- weights_one: float32 [4, 16384], P('merge'), may hold values from 0.003 to 32, as said below
- roots_one: float32 [4, 16384], P('merge'), may hold values from -2047.55 to 2048.85, as said below
- live_two: int32 [4], replicated, may hold values from 2048 to 6144, as said below
- order_two: int32 [4, 16384], P('merge'), may hold values from 0 to 16383, each once within a row
- poles_two: float32 [4, 16384], P('merge'), may hold values from -2048 to 2048.3, as said below
- weights_two: float32 [4, 16384], P('merge'), may hold values from 0.003 to 32, as said below
- roots_two: float32 [4, 16384], P('merge'), may hold values from -2047.55 to 2048.85, as said below
Outputs:
- vectors_two: bfloat16 [4, 128, 32768], P('merge', 'row', 'col')
The draws below stay inside these ranges and needn't reach their ends.
Inputs may be any that keep to these rules, and one draw needn't show every extreme that they name: `live_one`: both ends of the range are reached in every draw. `live_two`: both ends of the range are reached in every draw. `weights_one`: Positive. `weights_two`: Positive. `poles_one`: every offset minus its floor lies in [0, 0.3]. `roots_one`: every offset minus its floor lies in [0.45, 0.85], so every root stays 0.15 or more from every pole. `poles_two`: every offset minus its floor lies in [0, 0.3]. `roots_two`: every offset minus its floor lies in [0.45, 0.85], so every root stays 0.15 or more from every pole.
All inputs are finite; a program needn't handle non-finite values.
Results may differ from the reference program's by a relative error of at most 0.0031.
Values may be sent and summed in bfloat16 or wider, within the bound.
No kernel may reach another device: no remote copies, remote signals or barrier semaphores. Data moves between devices by JAX's collectives and lax.ppermute only.
A program may use at most 64 MiB of HBM per device.

```python
import math
import jax
import jax.numpy as jnp
from jax import lax

MERGE_ORDER = 16384
ROWS = 128
N_MERGE = 4


def count_law(key):
    first_key, second_key, third_key = jax.random.split(key, 3)
    counts = jax.random.randint(first_key, (N_MERGE,), MERGE_ORDER // 8, 3 * MERGE_ORDER // 8 + 1)
    highest = jax.random.randint(second_key, (), 0, N_MERGE)
    lowest = (highest + 1 + jax.random.randint(third_key, (), 0, N_MERGE - 1)) % N_MERGE
    numbers = jnp.arange(N_MERGE)
    counts = jnp.where(numbers == highest, 3 * MERGE_ORDER // 8, counts)
    counts = jnp.where(numbers == lowest, MERGE_ORDER // 8, counts)
    return counts.astype(jnp.int32)


def weight_law(key):
    scale_key, phase_key = jax.random.split(key)
    scaled = jnp.exp(jax.random.uniform(scale_key, (N_MERGE, MERGE_ORDER), jnp.float32, math.log(0.1), 0.0))
    phases = jax.random.uniform(phase_key, (N_MERGE, 1), jnp.float32, 0.0, 2.0 * math.pi)
    slots = jnp.arange(MERGE_ORDER).astype(jnp.float32)
    swing = 0.5
    period = 1024.0
    return scaled * jnp.exp(math.log(10.0) * swing * jnp.sin(2.0 * math.pi * slots / period + phases))


def offset_law(key, lowest, highest):
    fraction_key = jax.random.fold_in(key, 0)
    fraction = jax.random.uniform(fraction_key, (N_MERGE, MERGE_ORDER), jnp.float32, lowest, highest)
    return fraction


def draw_live_one(key, part):
    return count_law(jax.random.fold_in(key, 11))


def draw_live_two(key, part):
    return count_law(jax.random.fold_in(key, 23))


def draw_weights_one(key, part):
    return weight_law(jax.random.fold_in(key, 37))


def draw_weights_two(key, part):
    return weight_law(jax.random.fold_in(key, 41))


def draw_poles_one(key, part):
    return offset_law(jax.random.fold_in(key, 53), 0.0, 0.3)


def draw_roots_one(key, part):
    return offset_law(jax.random.fold_in(key, 59), 0.45, 0.85)


def draw_poles_two(key, part):
    return offset_law(jax.random.fold_in(key, 61), 0.0, 0.3)


def draw_roots_two(key, part):
    return offset_law(jax.random.fold_in(key, 67), 0.45, 0.85)


def block_scale(own_key, shape, cuts, smallest, top_value):
    factor_of = 1.0
    for axis_at, parts in cuts:
        draws = jax.random.uniform(jax.random.fold_in(jax.random.fold_in(own_key, 6), axis_at), (parts,), jnp.float32, smallest / len(cuts), top_value / len(cuts))
        factor_of = factor_of * jnp.repeat(jnp.exp(draws), shape[axis_at] // parts).reshape((-1,) + (1,) * (len(shape) - 1 - axis_at))
    return factor_of


def centred(stream_key, shape, scale, limit, cuts=(), kind=jnp.bfloat16):
    values = scale * jax.random.normal(stream_key, shape, jnp.float32)
    if cuts:
        values = values * block_scale(stream_key, shape, cuts, -0.22, 0.18)
    return jnp.clip(values, -limit, limit).astype(kind)


def setup_inputs(seed: int = 0) -> dict:
    streams_of = jax.random.split(jax.random.key(seed), 12)
    eigen_rows = centred(streams_of[0], (N_MERGE, ROWS, MERGE_ORDER), 1.0, 6.0, ((0, 4), (1, 4), (2, 16)))
    live_one = draw_live_one(jax.random.fold_in(streams_of[11], 71), 0)
    order_one = jax.vmap(lambda own: jax.random.permutation(own, MERGE_ORDER))(jax.random.split(streams_of[2], N_MERGE)).reshape((N_MERGE, MERGE_ORDER)).astype(jnp.int32)
    poles_one = draw_poles_one(jax.random.fold_in(streams_of[11], 71), 0)
    weights_one = draw_weights_one(jax.random.fold_in(streams_of[11], 71), 0)
    roots_one = draw_roots_one(jax.random.fold_in(streams_of[11], 71), 0)
    live_two = draw_live_two(jax.random.fold_in(streams_of[11], 71), 0)
    order_two = jax.vmap(lambda own: jax.random.permutation(own, MERGE_ORDER))(jax.random.split(streams_of[7], N_MERGE)).reshape((N_MERGE, MERGE_ORDER)).astype(jnp.int32)
    poles_two = draw_poles_two(jax.random.fold_in(streams_of[11], 71), 0)
    weights_two = draw_weights_two(jax.random.fold_in(streams_of[11], 71), 0)
    roots_two = draw_roots_two(jax.random.fold_in(streams_of[11], 71), 0)
    return {"eigen_rows": eigen_rows, "live_one": live_one, "order_one": order_one, "poles_one": poles_one, "weights_one": weights_one, "roots_one": roots_one, "live_two": live_two, "order_two": order_two, "poles_two": poles_two, "weights_two": weights_two, "roots_two": roots_two}


column_block = 512

def square_sums(source_place, source_shift, source_weight, live_rows, column_place, column_shift):
    numbers = jnp.arange(source_place.shape[0], dtype=jnp.int32)
    squares = jnp.where(numbers < live_rows, source_weight * source_weight, 0.0)

    def one_block(pieces):
        places, shifts = pieces
        distance = source_place[:, None] - places[None, :] + (source_shift[:, None] - shifts[None, :])
        return lax.optimization_barrier(jnp.sum(squares[:, None] / (distance * distance), axis=0))
    blocks = lax.map(one_block, (column_place.reshape(-1, column_block), column_shift.reshape(-1, column_block)))
    return blocks.reshape(-1)

def apply_cauchy(permuted, source_place, source_shift, source_weight, live_rows, column_place, column_shift, inverse_norm, live_columns):
    numbers = jnp.arange(source_place.shape[0], dtype=jnp.int32)
    row_keep = numbers < live_rows
    columns = jnp.arange(column_place.shape[0], dtype=jnp.int32)

    def one_block(pieces):
        places, shifts, inverse, indices = pieces
        distance = source_place[:, None] - places[None, :] + (source_shift[:, None] - shifts[None, :])
        entries = source_weight[:, None] / distance * inverse[None, :]
        entries = jnp.where(row_keep[:, None] & (indices < live_columns)[None, :], entries, 0.0)
        rounded = lax.optimization_barrier(entries.astype(jnp.bfloat16)).astype(jnp.float32)
        return jnp.dot(permuted, rounded, precision=lax.Precision.HIGHEST)
    blocks = lax.map(one_block, (column_place.reshape(-1, column_block), column_shift.reshape(-1, column_block), inverse_norm.reshape(-1, column_block), columns.reshape(-1, column_block)))
    return jnp.transpose(blocks, (1, 0, 2)).reshape(permuted.shape[0], -1)

def reference(eigen_rows, live_one, order_one, poles_one, weights_one, roots_one, live_two, order_two, poles_two, weights_two, roots_two):
    merge_order = order_one.shape[1]
    slots = jnp.arange(merge_order, dtype=jnp.int32)
    level_list = []
    for merge_number in range(N_MERGE):
        live_level = live_one[merge_number]
        permuted = jnp.take(eigen_rows[merge_number].astype(jnp.float32), order_one[merge_number], axis=1)
        places = slots.astype(jnp.float32)
        sums = square_sums(places, poles_one[merge_number], weights_one[merge_number], live_level, places, roots_one[merge_number])
        inverse = 1.0 / jnp.sqrt(sums)
        cauchy = apply_cauchy(permuted, places, poles_one[merge_number], weights_one[merge_number], live_level, places, roots_one[merge_number], inverse, live_level)
        level_list.append(jnp.where(slots[None, :] < live_level, cauchy, permuted).astype(jnp.bfloat16))
    columns = jnp.arange(2 * merge_order, dtype=jnp.int32)
    outputs = []
    for pair_number in range(N_MERGE // 2):
        first_merge = 2 * pair_number
        second_merge = first_merge + 1
        count_first = live_two[first_merge]
        count_second = live_two[second_merge]
        joined = count_first + count_second
        from_first = columns < count_first
        slot_index = jnp.clip(jnp.where(from_first, columns, columns - count_first), 0, merge_order - 1)
        column_place = (2 * slot_index + jnp.where(from_first, 0, 1)).astype(jnp.float32)
        column_shift = jnp.where(from_first, jnp.take(roots_two[first_merge], slot_index), jnp.take(roots_two[second_merge], slot_index))
        sums = square_sums((2 * slots).astype(jnp.float32), poles_two[first_merge], weights_two[first_merge], count_first, column_place, column_shift)
        sums = sums + square_sums((2 * slots + 1).astype(jnp.float32), poles_two[second_merge], weights_two[second_merge], count_second, column_place, column_shift)
        inverse = 1.0 / jnp.sqrt(sums)
        for half_index in range(2):
            merge_number = first_merge + half_index
            permuted = jnp.take(level_list[merge_number].astype(jnp.float32), order_two[merge_number], axis=1)
            cauchy = apply_cauchy(permuted, (2 * slots + half_index).astype(jnp.float32), poles_two[merge_number], weights_two[merge_number], live_two[merge_number], column_place, column_shift, inverse, joined)
            extra = columns - joined
            first_source = extra < merge_order - count_first
            if half_index == 0:
                own_source = first_source
                position = count_first + extra
            else:
                own_source = jnp.logical_not(first_source)
                position = count_second + extra - (merge_order - count_first)
            position = jnp.clip(position, 0, merge_order - 1).astype(jnp.int32)
            moved = jnp.where(own_source[None, :], jnp.take(permuted, position, axis=1), 0.0)
            outputs.append(jnp.where(columns[None, :] < joined, cauchy, moved).astype(jnp.bfloat16))
    return jnp.stack(outputs)
```

```python
import jax
import jax.numpy as jnp
from jax import lax
from jax.experimental import pallas as pl
from jax.experimental.pallas import tpu as pltpu
from jax.sharding import PartitionSpec as P

F32 = jnp.float32
BF16 = jnp.bfloat16
NT = (((1,), (1,)), ((), ()))
NN = (((1,), (0,)), ((), ()))


def params(mib=56):
    return pltpu.CompilerParams(vmem_limit_bytes=mib * 1024 * 1024)


def lane_iota(rows, columns):
    return lax.broadcasted_iota(jnp.int32, (rows, columns), 1)


def row_iota(rows, columns):
    return lax.broadcasted_iota(jnp.int32, (rows, columns), 0)


def down_lanes(row):
    return jnp.broadcast_to(row, (128, 128)).T


def halves(value):
    first = value.astype(BF16).astype(F32)
    return first, value - first


def place_poles_kernel(meta, order, poles, weights, out, total):
    live = meta[0]
    total[...] = jnp.zeros_like(total)

    def step(turn, carry):
        parts = []
        for half in range(2):
            row = turn * 2 + half
            number = row * 128 + lane_iota(1, 128)
            keep = number < live
            column = jnp.where(keep, order[pl.ds(row, 1), :], -1)
            pole = poles[pl.ds(row, 1), :]
            weight = weights[pl.ds(row, 1), :]
            whole = jnp.floor(pole)
            place = number.astype(F32) + whole
            high = jnp.floor(place * (1.0 / 128.0))
            parts.append(
                (column >> 7, column & 127, high, place - 128.0 * high)
                + halves(pole - whole)
                + halves(weight)
            )
        joined = [jnp.concatenate([a, b], axis=1) for a, b in zip(*parts)]
        rows = row_iota(128, 256)
        hot_high = rows == joined[0]
        hot_low = jnp.where(rows == joined[1], 1.0, 0.0).astype(BF16)
        left = jnp.concatenate(
            [jnp.where(hot_high, value, 0.0).astype(BF16) for value in joined[2:]], axis=0
        )
        total[...] += lax.dot_general(left, hot_low, NT, preferred_element_type=F32)
        return carry

    lax.fori_loop(0, (live + 255) // 256, step, 0)
    out[0] = total[0:128] * 128.0 + total[128:256]
    out[1] = total[256:384] + total[384:512]
    out[2] = total[512:640] + total[640:768]


def level_one_kernel(meta, table, poles, weights, roots, out, place, inverse):
    live = meta[0]
    panels = place.shape[0] // 128
    first = meta[6] * (panels * 128)
    centre = (first + panels * 64).astype(F32)

    @pl.when(pl.program_id(0) == 0)
    def _():
        for panel in range(panels):
            root = roots[pl.ds(meta[6] * panels + panel, 1), :]
            whole = jnp.floor(root)
            number = (first + panel * 128 + lane_iota(1, 128)).astype(F32)
            spread = down_lanes((number + whole - centre) + (root - whole))
            place[panel * 128 : panel * 128 + 128, :] = spread

            def add(row, running):
                pole = poles[pl.ds(row, 1), :]
                weight = weights[pl.ds(row, 1), :]
                numbers = row * 128 + lane_iota(1, 128)
                down = jnp.floor(pole)
                pole_place = (numbers.astype(F32) + down - centre) + (pole - down)
                square = jnp.where(numbers < live, weight * weight, 0.0)
                distance = pole_place - spread
                return running + square / (distance * distance)

            sums = lax.fori_loop(0, (live + 127) // 128, add, jnp.zeros((128, 128), F32))
            scale = 1.0 / jnp.sqrt(jnp.sum(sums, axis=1, keepdims=True))
            inverse[panel * 128 : panel * 128 + 128, :] = jnp.broadcast_to(scale, (128, 128))

    base = pl.program_id(0) * 8
    for chunk in range(8):
        pole_place = (table[0, pl.ds(base + chunk, 1), :] - centre) + table[
            1, pl.ds(base + chunk, 1), :
        ]
        weight = table[2, pl.ds(base + chunk, 1), :]
        for panel in range(panels):
            rows = slice(panel * 128, panel * 128 + 128)
            entries = weight / (pole_place - place[rows, :]) * inverse[rows, :]
            out[rows, chunk * 128 : chunk * 128 + 128] = entries.astype(BF16)


def apply_one_kernel(cauchy, rows, out, total):
    @pl.when(pl.program_id(0) == 0)
    def _():
        total[...] = jnp.zeros_like(total)

    total[...] += lax.dot_general(cauchy[...], rows[0], NT, preferred_element_type=F32)

    @pl.when(pl.program_id(0) == pl.num_programs(0) - 1)
    def _():
        out[...] = total[...].T.astype(BF16)


def level_two_kernel(meta, centres, poles, weights, places, out, sums):
    live = meta[1]
    block = pl.program_id(0)
    active = meta[6] * out.shape[0] * pl.num_programs(0) + block * 128 < meta[2]
    chunks = jnp.where(active, (live + 255) // 256 * 2, 0)
    spread = down_lanes(places[pl.ds(block, 1), :])
    centre = centres[block]

    def step(row, running):
        pole = poles[pl.ds(row, 1), :]
        numbers = row * 128 + lane_iota(1, 128)
        whole = jnp.floor(pole)
        pole_place = ((2 * numbers + meta[5]).astype(F32) + whole - centre) + (pole - whole)
        weight = jnp.where(numbers < live, weights[pl.ds(row, 1), :], 0.0)
        entries = weight / (pole_place - spread)
        out[:, pl.ds(pl.multiple_of(row * 128, 128), 128)] = entries.astype(BF16)
        return running + entries * entries

    total = lax.fori_loop(0, chunks, step, jnp.zeros((128, 128), F32))
    sums[0] = jnp.sum(total.T, axis=0, keepdims=True)


def apply_two_kernel(
    meta, first_order, second_order, cauchy, raw, solved, norms, out, table, picked, source, moved
):
    live_one = meta[0]
    live_two = meta[1]
    joined = meta[2]
    merge_order = raw.shape[0] * raw.shape[2]
    solved_total = solved.shape[0] * solved.shape[2]
    width = moved.shape[0]
    block_width = out.shape[2]
    start = meta[6] * width
    turns = (live_two + 255) // 256

    def row_of(number):
        level = second_order[number]
        return jnp.where(level < live_one, level, solved_total + first_order[level])

    @pl.when(pl.program_id(0) == 0)
    def _():
        def lay_raw(block, carry):
            for part in range(raw.shape[2] // 128):
                at = solved_total + block * raw.shape[2] + part * 128
                table[pl.ds(pl.multiple_of(at, 128), 128), 0:32] = (
                    raw[block, :, part * 128 : part * 128 + 128].astype(F32).T
                )
            return carry

        lax.fori_loop(0, raw.shape[0], lay_raw, 0)

        def lay_solved(block, carry):
            for part in range(solved.shape[2] // 128):
                at = block * solved.shape[2] + part * 128
                table[pl.ds(pl.multiple_of(at, 128), 128), 0:32] = (
                    solved[block, :, part * 128 : part * 128 + 128].astype(F32).T
                )
            return carry

        lax.fori_loop(0, solved.shape[0], lay_solved, 0)

        @pl.when(start < joined)
        def _():
            def pick(turn, carry):
                for part in range(16):
                    at = turn * 16 + part
                    picked[pl.ds(at, 1), :] = table[pl.ds(row_of(at), 1), :]
                return carry

            lax.fori_loop(0, turns * 16, pick, 0)

            def narrow(turn, carry):
                rows = pl.ds(pl.multiple_of(turn * 256, 256), 256)
                source[rows, :] = picked[rows, :].astype(BF16)
                return carry

            lax.fori_loop(0, turns, narrow, 0)

        @pl.when(start + width > joined)
        def _():
            def move(turn, carry):
                for part in range(16):
                    at = turn * 16 + part
                    number = jnp.clip(meta[7] + at, 0, merge_order - 1)
                    moved[pl.ds(at, 1), :] = table[pl.ds(row_of(number), 1), :]
                return carry

            lax.fori_loop(0, width // 16, move, 0)

    here = start + pl.program_id(0) * block_width
    depth = jnp.where(here < joined, turns, 0)

    def step(turn, running):
        at = pl.ds(pl.multiple_of(turn * 256, 256), 256)
        return running + lax.dot_general(
            cauchy[:, at], source[at, :], NN, preferred_element_type=F32
        )

    total = lax.fori_loop(0, depth, step, jnp.zeros((block_width, 128), F32))
    for part in range(block_width // 128):
        number = here + part * 128 + lane_iota(1, 128)
        number = jnp.broadcast_to(number, (32, 128))
        first_part = number - joined < merge_order - meta[3]
        own = jnp.where(meta[5] == 0, first_part.astype(jnp.int32), 1 - first_part.astype(jnp.int32))
        solved_part = total[part * 128 : part * 128 + 128, :].T[0:32, :]
        norm = norms[pl.ds(pl.program_id(0) * (block_width // 128) + part, 1), :]
        solved_part = solved_part * (1.0 / jnp.sqrt(norm))
        at = pl.multiple_of(pl.program_id(0) * block_width + part * 128, 128)
        moved_part = moved[pl.ds(at, 128), :].T[0:32, :]
        moved_part = jnp.where(own == 1, moved_part, 0.0)
        out[0, :, part * 128 : part * 128 + 128] = jnp.where(
            number < joined, solved_part, moved_part
        ).astype(BF16)


SMEM = pltpu.SMEM
VMEM = pltpu.VMEM


def whole(space=VMEM):
    return pl.BlockSpec(memory_space=space)


def send_to_all(array, axis):
    size = lax.axis_size(axis)
    return lax.all_to_all(
        jnp.broadcast_to(array[None], (size, *array.shape)), axis, 0, 0, tiled=True
    )


def cost(flops):
    return pl.CostEstimate(flops=flops, bytes_accessed=1000000, transcendentals=0)


def partner(value, axis):
    pairs = [(source, source ^ 1) for source in range(lax.axis_size(axis))]
    return lax.ppermute(value, axis, pairs)


def shards(
    eigen_rows,
    live_one,
    order_one,
    poles_one,
    weights_one,
    roots_one,
    live_two,
    order_two,
    poles_two,
    weights_two,
    roots_two,
):
    col_count = lax.axis_size("col")
    col = lax.axis_index("col")
    merge = lax.axis_index("merge")
    row_total, local_columns = eigen_rows.shape[1:]
    merge_order = order_one.shape[1]
    live_most = merge_order * 3 // 8
    live_rows = live_most // 128
    one_width = live_most // col_count
    width = 2 * merge_order // col_count
    panels = width // 128
    half = merge % 2
    first = merge - half
    count_first = live_two[first]
    count_second = live_two[first + 1]
    joined = count_first + count_second
    moved_from = col * width - joined
    moved_from = moved_from + jnp.where(
        half == 0, count_first, count_second - (merge_order - count_first)
    )
    meta = jnp.stack(
        [
            live_one[merge],
            live_two[merge],
            joined,
            count_first,
            count_second,
            half,
            col,
            moved_from,
        ]
    ).astype(jnp.int32)

    def rows_of(array):
        return array[0, :live_most].reshape(live_rows, 128)

    raw = send_to_all(eigen_rows[0], "col")
    other_roots = partner(roots_two[0], "merge")

    table = pl.pallas_call(
        place_poles_kernel,
        out_shape=jax.ShapeDtypeStruct((3, 128, 128), F32),
        in_specs=[whole(SMEM), whole(), whole(), whole()],
        out_specs=whole(),
        scratch_shapes=[VMEM((6 * 128, 128), F32)],
        compiler_params=params(),
        cost_estimate=cost(10**9),
        name="place_poles",
    )(meta, rows_of(order_one), rows_of(poles_one), rows_of(weights_one))

    cauchy_one = pl.pallas_call(
        level_one_kernel,
        out_shape=jax.ShapeDtypeStruct((one_width, merge_order), BF16),
        grid=(merge_order // 1024,),
        in_specs=[whole(SMEM), whole(), whole(), whole(), whole()],
        out_specs=pl.BlockSpec((one_width, 1024), lambda step: (0, step)),
        scratch_shapes=[VMEM((one_width, 128), F32), VMEM((one_width, 128), F32)],
        compiler_params=params(),
        cost_estimate=cost(10**9),
        name="level_one",
    )(meta, table, rows_of(poles_one), rows_of(weights_one), roots_one.reshape(-1, 128))

    roots_first = jnp.where(half == 0, roots_two[0], other_roots)
    roots_second = jnp.where(half == 0, other_roots, roots_two[0])
    columns = col * width + jnp.arange(width, dtype=jnp.int32)
    from_first = columns < count_first
    slot = jnp.where(from_first, columns, columns - count_first)
    padded = jnp.concatenate([jnp.zeros((merge_order,), F32), roots_second])
    root = jnp.where(
        from_first,
        lax.dynamic_slice(roots_first, (col * width,), (width,)),
        lax.dynamic_slice(padded, (merge_order + col * width - count_first,), (width,)),
    )
    place = (2 * slot + jnp.where(from_first, 0, 1)).astype(F32).reshape(panels, 128)
    root = root.reshape(panels, 128)
    centres = place[:, 0]
    lowest = jnp.floor(root)
    places = (place + lowest - centres[:, None]) + (root - lowest)

    cauchy_two, sums = pl.pallas_call(
        level_two_kernel,
        out_shape=(
            jax.ShapeDtypeStruct((width, live_most), BF16),
            jax.ShapeDtypeStruct((panels, 1, 128), F32),
        ),
        grid=(panels,),
        in_specs=[whole(SMEM), whole(SMEM), whole(), whole(), whole()],
        out_specs=(
            pl.BlockSpec((128, live_most), lambda step: (step, 0)),
            pl.BlockSpec((1, 1, 128), lambda step: (step, 0, 0)),
        ),
        compiler_params=params(),
        cost_estimate=cost(2 * 10**9),
        name="level_two",
    )(meta, centres, rows_of(poles_two), rows_of(weights_two), places)
    sums = sums.reshape(panels, 128)
    norms = sums + partner(sums, "merge")

    solved = pl.pallas_call(
        apply_one_kernel,
        out_shape=jax.ShapeDtypeStruct((row_total, one_width), BF16),
        grid=(col_count,),
        in_specs=[
            pl.BlockSpec((one_width, local_columns), lambda step: (0, step)),
            pl.BlockSpec((1, row_total, local_columns), lambda step: (step, 0, 0)),
        ],
        out_specs=pl.BlockSpec((row_total, one_width), lambda step: (0, 0)),
        scratch_shapes=[VMEM((one_width, row_total), F32)],
        compiler_params=params(),
        cost_estimate=cost(10**9),
        name="apply_one",
    )(cauchy_one, raw)
    solved = send_to_all(solved, "col")

    block_width = 512
    result = pl.pallas_call(
        apply_two_kernel,
        out_shape=jax.ShapeDtypeStruct((1, row_total, width), BF16),
        grid=(width // block_width,),
        in_specs=[
            whole(SMEM),
            whole(SMEM),
            whole(SMEM),
            pl.BlockSpec((block_width, live_most), lambda step: (step, 0)),
            whole(),
            whole(),
            whole(),
        ],
        out_specs=pl.BlockSpec((1, row_total, block_width), lambda step: (0, 0, step)),
        scratch_shapes=[
            VMEM((live_most + merge_order, 128), F32),
            VMEM((live_most, 128), F32),
            VMEM((live_most, 128), BF16),
            VMEM((width, 128), F32),
        ],
        compiler_params=params(),
        cost_estimate=cost(10**9),
        name="apply_two",
    )(meta, order_one[0], order_two[0], cauchy_two, raw, solved, norms)
    return result


def solution(mesh):
    placed = (
        P("merge", "row", "col"),
        P(),
        P("merge", None),
        P("merge", None),
        P("merge", None),
        P("merge", None),
        P(),
        P("merge", None),
        P("merge", None),
        P("merge", None),
        P("merge", None),
    )
    return jax.shard_map(
        shards, mesh=mesh, in_specs=placed, out_specs=P("merge", "row", "col"), check_vma=False
    )
```
